32 devices in a mesh: outer: 4 (over y, x), inner: 8 (over z, core).
Axes of the slice: x: 2, y: 2, z: 4, core: 2. Of those that a mesh axis runs over, the one named last changes fastest.
Arguments:
- queries: bfloat16 [2048, 1024], P(('outer', 'inner')), may hold values from -8 to 8
- key_rows: bfloat16 [2048, 1024], P(('outer', 'inner')), may hold values from -8 to 8
- value_rows: bfloat16 [2048, 1024], P(('outer', 'inner')), may hold values from -6 to 6
Outputs:
- attended: float32 [2048, 1024], P(('outer', 'inner'))
The draws below stay inside these ranges and needn't reach their ends.
All inputs are finite; a program needn't handle non-finite values.
Results may differ from the reference program's by a relative error of at most 0.0021.
Values may be sent and summed in bfloat16 or wider, within the bound.
A program may use at most 64 MiB of HBM per device.

```python
from functools import reduce
import jax
import jax.numpy as jnp
import numpy as np
from jax import lax

HEADS = 16
HEAD_DIM = 64
TOK_DEV = 64
GROUP_LEN = 512
SEQUENCE = 2048


def draw_queries(key, part):
    shape = (SEQUENCE, HEADS * HEAD_DIM)
    base = jax.random.truncated_normal(jax.random.fold_in(key, 1), -6.0, 6.0, shape, jnp.float32)
    return base.astype(jnp.bfloat16)


def draw_key_rows(key, part):
    shape = (SEQUENCE, HEADS * HEAD_DIM)
    base = jax.random.truncated_normal(jax.random.fold_in(key, 2), -6.0, 6.0, shape, jnp.float32)
    return base.astype(jnp.bfloat16)


def block_levels(key, extent, cuts, smallest, top_value):
    def one(axis_at, blocks):
        heights = jax.random.uniform(jax.random.fold_in(jax.random.fold_in(key, 6), axis_at), (blocks,), jnp.float32, smallest / len(cuts), top_value / len(cuts))
        return jnp.repeat(jnp.exp(heights), extent[axis_at] // blocks).reshape((-1,) + (1,) * (len(extent) - axis_at - 1))

    loudness = one(*cuts[0])
    for cut in cuts[1:]:
        loudness = loudness * one(*cut)
    return loudness


def gaussian(key, shape, scale, reach, split=(), kind=jnp.bfloat16):
    gain = block_levels(key, shape, split, -0.22, 0.18) if split else 1.0
    values = jax.random.normal(key, shape, jnp.float32) * scale * gain
    return jnp.minimum(jnp.maximum(values, -reach), reach).astype(kind)


def setup_inputs(seed: int = 0) -> dict:
    key_list = jax.random.split(jax.random.key(seed), 4)
    return {
        "queries": draw_queries(jax.random.fold_in(key_list[3], 71), 0),
        "key_rows": draw_key_rows(jax.random.fold_in(key_list[3], 71), 0),
        "value_rows": gaussian(key_list[2], (SEQUENCE, HEADS * HEAD_DIM), 1.0, 6.0, ((0, 32),)),
    }


FLOOR_SCORE = -1.0e30


def dense_causal(query_rows, key_rows, value_rows, ranks):
    scale = HEAD_DIM ** -0.5
    scores = jnp.dot(query_rows.astype(jnp.float32), key_rows.astype(jnp.float32).T, precision=lax.Precision.HIGHEST) * scale
    scores = jnp.where(ranks[None, :] <= ranks[:, None], scores, FLOOR_SCORE)
    row_max = jnp.max(scores, axis=1)
    weights = jnp.exp(scores - row_max[:, None])
    denominator = jnp.sum(weights, axis=1)
    rounded = lax.optimization_barrier(weights.astype(jnp.bfloat16)).astype(jnp.float32)
    summed = jnp.dot(rounded, value_rows.astype(jnp.float32), precision=lax.Precision.HIGHEST)
    return summed / denominator[:, None], row_max + jnp.log(denominator)


def level_one(queries, key_rows, value_rows):
    blocks = SEQUENCE // TOK_DEV
    ranks = jnp.arange(TOK_DEV, dtype=jnp.int32)

    def one_block(pieces):
        return jax.vmap(dense_causal, in_axes=(1, 1, 1, None), out_axes=(1, 1))(pieces[0], pieces[1], pieces[2], ranks)

    shaped = tuple(a.reshape(blocks, TOK_DEV, HEADS, HEAD_DIM) for a in (queries, key_rows, value_rows))
    outputs, lses = lax.map(one_block, shaped)
    return outputs.reshape(SEQUENCE, HEADS, HEAD_DIM), lses.reshape(SEQUENCE, HEADS)


def level_two(queries, key_rows, value_rows):
    groups = SEQUENCE // GROUP_LEN
    class_len = GROUP_LEN // 4
    ranks = jnp.arange(class_len, dtype=jnp.int32)

    def regroup(array):
        return array.reshape(groups, class_len, 4, HEADS, HEAD_DIM).transpose(0, 3, 2, 1, 4).reshape(groups * HEADS * 4, class_len, HEAD_DIM)

    def one_item(pieces):
        return dense_causal(pieces[0], pieces[1], pieces[2], ranks)

    outputs, lses = lax.map(one_item, (regroup(queries), regroup(key_rows), regroup(value_rows)))
    outputs = outputs.reshape(groups, HEADS, 4, class_len, HEAD_DIM).transpose(0, 3, 2, 1, 4).reshape(SEQUENCE, HEADS, HEAD_DIM)
    lses = lses.reshape(groups, HEADS, 4, class_len).transpose(0, 3, 2, 1).reshape(SEQUENCE, HEADS)
    return outputs, lses


def level_three(queries, key_rows, value_rows):
    sixteenth = SEQUENCE // 16
    pick = np.array([head * 16 + (head // 4) * 4 + residue for head in range(HEADS) for residue in range(4)], np.int32)
    ranks = jnp.arange(sixteenth, dtype=jnp.int32)

    def regroup(array):
        spread = array.reshape(sixteenth, 16, HEADS, HEAD_DIM).transpose(2, 1, 0, 3).reshape(HEADS * 16, sixteenth, HEAD_DIM)
        return jnp.take(spread, pick, axis=0)

    def one_item(pieces):
        return dense_causal(pieces[0], pieces[1], pieces[2], ranks)

    outputs, lses = lax.map(one_item, (regroup(queries), regroup(key_rows), regroup(value_rows)))
    full_out = jnp.zeros((HEADS * 16, sixteenth, HEAD_DIM), jnp.float32).at[pick].set(outputs)
    full_lse = jnp.full((HEADS * 16, sixteenth), FLOOR_SCORE, jnp.float32).at[pick].set(lses)
    full_out = full_out.reshape(HEADS, 16, sixteenth, HEAD_DIM).transpose(2, 1, 0, 3).reshape(SEQUENCE, HEADS, HEAD_DIM)
    full_lse = full_lse.reshape(HEADS, 16, sixteenth).transpose(2, 1, 0).reshape(SEQUENCE, HEADS)
    return full_out, full_lse


def merge_levels(parts):
    row_max = reduce(jnp.maximum, [lse for _, lse in parts])
    weights = [jnp.exp(lse - row_max) for _, lse in parts]
    denominator = reduce(jnp.add, weights)
    summed = reduce(jnp.add, [weight[..., None] * output for weight, (output, _) in zip(weights, parts)])
    return summed / denominator[..., None], row_max + jnp.log(denominator)


def reference(queries, key_rows, value_rows):
    shaped = tuple(a.reshape(SEQUENCE, HEADS, HEAD_DIM) for a in (queries, key_rows, value_rows))
    first = level_one(*shaped)
    second = level_two(*shaped)
    third = level_three(*shaped)
    combined, _ = merge_levels([first, second, third])
    return combined.reshape(SEQUENCE, HEADS * HEAD_DIM)
```

```python
import math
from functools import partial, reduce

import jax
import jax.numpy as jnp
import numpy as np
from jax import lax
from jax.experimental import pallas as pl
from jax.experimental.pallas import tpu as pltpu
from jax.sharding import PartitionSpec as P

HEADS = 16


FLOOR_SCORE = -1e30


def divisor_block(length, limit):
    extent = min(length, limit)
    while length % extent:
        extent -= 1
    return extent


def fresh_state(count, rows, width):
    return (
        jnp.full((count, rows), FLOOR_SCORE, jnp.float32),
        jnp.zeros((count, rows), jnp.float32),
        jnp.zeros((count, rows, width), jnp.float32),
    )


def finish_state(state):
    row_max, denominator, summed = state
    return (summed / denominator[..., None], row_max + jnp.log(denominator))


def online_step(state, query_rows, query_rank, key_rows, value_rows, key_rank):
    row_max, denominator, summed = state
    scale = query_rows.shape[-1] ** (-0.5)
    scores = (
        jnp.einsum("inh,ibh->inb", query_rows, key_rows, preferred_element_type=jnp.float32) * scale
    )
    scores = jnp.where(key_rank[None, None, :] <= query_rank[None, :, None], scores, FLOOR_SCORE)
    new_max = jnp.maximum(row_max, jnp.max(scores, axis=2))
    weights = jnp.exp(scores - new_max[..., None])
    rescale = jnp.exp(row_max - new_max)
    denominator = denominator * rescale + jnp.sum(weights, axis=2)
    summed = summed * rescale[..., None] + jnp.einsum(
        "inb,ibh->inh", weights.astype(jnp.bfloat16), value_rows, preferred_element_type=jnp.float32
    )
    return (new_max, denominator, summed)


def attend_keys(state, query_rows, query_rank, key_rows, value_rows, key_rank, stop=None):
    length = key_rows.shape[1]
    block = divisor_block(length, 512)

    def advance(index, carry):
        start = index * block
        piece_keys = lax.dynamic_slice_in_dim(key_rows, start, block, 1)
        piece_values = lax.dynamic_slice_in_dim(value_rows, start, block, 1)
        piece_rank = lax.dynamic_slice_in_dim(key_rank, start, block, 0)
        return online_step(carry, query_rows, query_rank, piece_keys, piece_values, piece_rank)

    upper = length // block if stop is None else stop
    return lax.fori_loop(0, upper, advance, state)


def attend(query_rows, query_rank, key_rows, value_rows, key_rank):
    count, length, width = query_rows.shape
    block = divisor_block(length, 512)
    steps = length // block
    query_split = query_rows.reshape(count, steps, block, width).swapaxes(0, 1)
    rank_split = query_rank.reshape(steps, block)

    def one_block(pieces):
        state = attend_keys(
            fresh_state(count, block, width),
            pieces[0],
            pieces[1],
            key_rows,
            value_rows,
            key_rank,
            pieces[2] + 1,
        )
        return finish_state(state)

    outputs, lses = lax.map(
        one_block, (query_split, rank_split, jnp.arange(steps, dtype=jnp.int32))
    )
    return (
        outputs.swapaxes(0, 1).reshape(count, length, width),
        lses.swapaxes(0, 1).reshape(count, length),
    )


def merge_levels(parts):
    row_max = reduce(jnp.maximum, [lse for _, lse in parts])
    weights = [jnp.exp(lse - row_max) for _, lse in parts]
    denominator = reduce(jnp.add, weights)
    summed = reduce(
        jnp.add, [weight[..., None] * output for weight, (output, _) in zip(weights, parts)]
    )
    return (summed / denominator[..., None], row_max + jnp.log(denominator))


def on_device(queries, key_rows, value_rows):
    tokens, features = queries.shape
    heads = HEADS
    width = features // heads
    outer_count = lax.axis_size("outer")
    inner_count = lax.axis_size("inner")
    outer_index = lax.axis_index("outer")
    inner_index = lax.axis_index("inner")
    per_device = 4 * heads // inner_count
    quarter = tokens // 4
    sixteenth = tokens // 16
    class_len = quarter * inner_count
    far_len = sixteenth * inner_count

    def to_items(array):
        return (
            array.reshape(quarter, 4, heads, width)
            .transpose(2, 1, 0, 3)
            .reshape(4 * heads, quarter, width)
        )

    local_ranks = jnp.arange(tokens, dtype=jnp.int32)
    head_major = [
        a.reshape(tokens, heads, width).transpose(1, 0, 2) for a in (queries, key_rows, value_rows)
    ]
    near_out, near_lse = attend(
        head_major[0], local_ranks, head_major[1], head_major[2], local_ranks
    )
    near_out = near_out.transpose(1, 0, 2)
    near_lse = near_lse.T
    item_index = inner_index * per_device + jnp.arange(per_device, dtype=jnp.int32)
    band = item_index // 16
    far_query_rank = outer_index * far_len + jnp.arange(far_len, dtype=jnp.int32)
    pick = np.array(
        [head * 16 + head // 4 * 4 + residue for head in range(heads) for residue in range(4)],
        np.int32,
    )

    def to_sixteen(array):
        spread = (
            array.reshape(sixteenth, 16, heads, width)
            .transpose(2, 1, 0, 3)
            .reshape(16 * heads, sixteenth, width)
        )
        return jnp.take(spread, pick, axis=0)

    gathered_k, gathered_v = (
        lax.all_gather(to_sixteen(key_rows), "outer", axis=1, tiled=True),
        lax.all_gather(to_sixteen(value_rows), "outer", axis=1, tiled=True),
    )
    mid_q, mid_k, mid_v, far_k, far_v = (
        lax.all_to_all(to_items(queries), "inner", split_axis=0, concat_axis=1, tiled=True),
        lax.all_to_all(to_items(key_rows), "inner", split_axis=0, concat_axis=1, tiled=True),
        lax.all_to_all(to_items(value_rows), "inner", split_axis=0, concat_axis=1, tiled=True),
        lax.all_to_all(gathered_k, "inner", split_axis=0, concat_axis=1, tiled=True),
        lax.all_to_all(gathered_v, "inner", split_axis=0, concat_axis=1, tiled=True),
    )
    split = mid_q.reshape(per_device, far_len, 4, width)
    picker = jnp.broadcast_to(band[:, None, None, None], (per_device, far_len, 1, width))
    far_q = jnp.take_along_axis(split, picker, axis=2)[:, :, 0, :]
    position = jnp.arange(far_k.shape[1], dtype=jnp.int32)
    far_key_rank = (
        position // sixteenth % outer_count * far_len
        + position // (outer_count * sixteenth) * sixteenth
        + position % sixteenth
    )
    far_state = attend_keys(
        fresh_state(per_device, far_len, width), far_q, far_query_rank, far_k, far_v, far_key_rank
    )
    far_out, far_lse = finish_state(far_state)
    class_ranks = jnp.arange(class_len, dtype=jnp.int32)
    mid_out, mid_lse = attend(mid_q, class_ranks, mid_k, mid_v, class_ranks)
    back_mid, back_mid_lse, back_far, back_far_lse = (
        lax.all_to_all(mid_out, "inner", split_axis=1, concat_axis=0, tiled=True),
        lax.all_to_all(mid_lse, "inner", split_axis=1, concat_axis=0, tiled=True),
        lax.all_to_all(far_out, "inner", split_axis=1, concat_axis=0, tiled=True),
        lax.all_to_all(far_lse, "inner", split_axis=1, concat_axis=0, tiled=True),
    )
    selector = np.array(
        [[band_index == head // 4 for band_index in range(4)] for head in range(heads)]
    )
    spread_out = jnp.where(
        selector[:, :, None, None, None], back_far.reshape(heads, 1, 4, sixteenth, width), 0.0
    )
    spread_lse = jnp.where(
        selector[:, :, None, None], back_far_lse.reshape(heads, 1, 4, sixteenth), FLOOR_SCORE
    )
    far_placed = (
        spread_out.reshape(heads, 16, sixteenth, width)
        .transpose(2, 1, 0, 3)
        .reshape(tokens, heads, width)
    )
    far_placed_lse = (
        spread_lse.reshape(heads, 16, sixteenth).transpose(2, 1, 0).reshape(tokens, heads)
    )
    placed = (
        back_mid.reshape(heads, 4, quarter, width)
        .transpose(2, 1, 0, 3)
        .reshape(tokens, heads, width)
    )
    placed_lse = back_mid_lse.reshape(heads, 4, quarter).transpose(2, 1, 0).reshape(tokens, heads)
    combined, _ = merge_levels(
        [(near_out, near_lse), (placed, placed_lse), (far_placed, far_placed_lse)]
    )
    return combined.reshape(tokens, features)


def fused_kernel(
    dims, q_ref, k_ref, v_ref, out_ref, q_buf, k_buf, v_buf, far_k, far_v, pick_k, pick_v, ready,
    in_send, in_recv, far_send, far_recv, back_send, back_recv, own_sem, own_back,
):
    inner, outer, tokens, slab, width, block = dims
    group = tokens * inner
    far_len = group // 4
    per_slab = slab // width
    me = lax.axis_index("inner")
    mine = lax.axis_index("outer")
    band = me * per_slab // 4
    sources = (k_ref, v_ref, q_ref)
    buffers = (k_buf, v_buf, q_buf)

    def columns(index):
        return pl.ds(pl.multiple_of(index * slab, slab), slab)

    def rows(index):
        return pl.ds(pl.multiple_of(index * tokens, tokens), tokens)

    def inbound(which, peer, owner):
        return pltpu.make_async_remote_copy(
            src_ref=sources[which].at[:, columns(peer)],
            dst_ref=buffers[which].at[rows(owner), :],
            send_sem=in_send.at[which, peer],
            recv_sem=in_recv.at[which, owner],
            device_id={"inner": peer},
            device_id_type=pl.DeviceIdType.MESH,
        )

    def farbound(which, peer, owner):
        return pltpu.make_async_remote_copy(
            src_ref=(pick_k, pick_v)[which],
            dst_ref=(far_k, far_v)[which].at[owner],
            send_sem=far_send.at[which, peer],
            recv_sem=far_recv.at[which, owner],
            device_id={"outer": peer},
            device_id_type=pl.DeviceIdType.MESH,
        )

    def backbound(peer, owner):
        return pltpu.make_async_remote_copy(
            src_ref=ready.at[rows(peer), :],
            dst_ref=out_ref.at[:, columns(owner)],
            send_sem=back_send.at[peer],
            recv_sem=back_recv.at[owner],
            device_id={"inner": peer},
            device_id_type=pl.DeviceIdType.MESH,
        )

    own_in = [
        pltpu.make_async_copy(
            sources[which].at[:, columns(me)], buffers[which].at[rows(me), :], own_sem.at[which]
        )
        for which in range(3)
    ]
    for copy in own_in:
        copy.start()
    barrier = pltpu.get_barrier_semaphore()
    for step in range(1, inner):
        pl.semaphore_signal(
            barrier, inc=1, device_id={"inner": lax.rem(me + step, inner)},
            device_id_type=pl.DeviceIdType.MESH,
        )
    for step in range(1, outer):
        pl.semaphore_signal(
            barrier, inc=1, device_id={"outer": lax.rem(mine + step, outer)},
            device_id_type=pl.DeviceIdType.MESH,
        )
    pl.semaphore_wait(barrier, inner + outer - 2)

    for which in range(3):
        for step in range(1, inner):
            inbound(which, lax.rem(me + step, inner), me).start()

    for other in range(outer - 1):

        @pl.when(mine <= other)
        def _():
            far_k[other] = jnp.zeros((far_len, slab), jnp.bfloat16)
            far_v[other] = jnp.zeros((far_len, slab), jnp.bfloat16)

    query_at = lax.broadcasted_iota(jnp.int32, (block, block), 0)
    key_at = lax.broadcasted_iota(jnp.int32, (block, block), 1)
    levels = (query_at % 4 == key_at % 4).astype(jnp.int32) + (
        (query_at % 16 == key_at % 16) & (query_at % 16 // 4 == band)
    ).astype(jnp.int32)

    def log_count(count):
        return jnp.where(
            count == 0,
            FLOOR_SCORE,
            jnp.where(count == 1, 0.0, jnp.where(count == 2, 1.0, math.log2(3.0))),
        )

    below = log_count(levels)
    diagonal = log_count(
        jnp.where(
            key_at <= query_at, levels + (query_at // tokens == key_at // tokens).astype(jnp.int32), 0
        )
    )
    far_query = lax.broadcasted_iota(jnp.int32, (block, far_len), 0)
    far_key = lax.broadcasted_iota(jnp.int32, (block, far_len), 1)
    far_one = jnp.where(far_query % 16 == 4 * band + far_key % 4, 0.0, FLOOR_SCORE)
    far_table = jnp.concatenate(
        [jnp.where(other < mine, far_one, FLOOR_SCORE) for other in range(outer - 1)], axis=1
    )
    picked = lax.broadcasted_iota(jnp.int32, (far_len, group), 0)
    picker = jnp.where(
        lax.broadcasted_iota(jnp.int32, (far_len, group), 1)
        == picked // 4 * 16 + 4 * band + picked % 4,
        1.0,
        0.0,
    ).astype(jnp.bfloat16)

    def arrive(which):
        own_in[which].wait()
        for step in range(1, inner):
            inbound(which, me, lax.rem(me + step, inner)).wait_recv()

    for which in range(2):
        arrive(which)
        (pick_k, pick_v)[which][...] = jnp.dot(
            picker, buffers[which][...], preferred_element_type=jnp.float32
        ).astype(jnp.bfloat16)
        for other in range(1, outer):

            @pl.when(mine < other)
            def _():
                farbound(which, other, mine).start()

    arrive(2)
    factor = width ** (-0.5) * math.log2(math.e)
    lane_head = lax.broadcasted_iota(jnp.int32, (block, slab), 1) // width
    contract = (((1,), (1,)), ((), ()))

    def query_of(index, head):
        piece = q_buf[index * block : (index + 1) * block, :]
        return jnp.where(lane_head == head, piece, jnp.zeros_like(piece))

    states = []
    for index in range(group // block):
        reach = (index + 1) * block
        table = jnp.concatenate([below] * index + [diagonal], axis=1)
        for head in range(per_slab):
            scores = lax.dot_general(
                query_of(index, head), k_buf[:reach, :], contract,
                preferred_element_type=jnp.float32,
            )
            scores = scores * factor + table
            top = jnp.max(scores, axis=1, keepdims=True)
            weights = jnp.exp2(scores - top)
            total = jnp.sum(weights, axis=1, keepdims=True)
            summed = jnp.dot(
                weights.astype(jnp.bfloat16), v_buf[:reach, :], preferred_element_type=jnp.float32
            )
            states.append((top, total, summed))

    for other in range(outer - 1):

        @pl.when(mine > other)
        def _():
            farbound(0, mine, other).wait_recv()
            farbound(1, mine, other).wait_recv()

    far_keys = far_k[...].reshape((outer - 1) * far_len, slab)
    far_values = far_v[...].reshape((outer - 1) * far_len, slab)
    for index in range(group // block):
        result = None
        for head in range(per_slab):
            top, total, summed = states[index * per_slab + head]
            scores = lax.dot_general(
                query_of(index, head), far_keys, contract, preferred_element_type=jnp.float32
            )
            scores = scores * factor + far_table
            new_top = jnp.maximum(top, jnp.max(scores, axis=1, keepdims=True))
            rescale = jnp.exp2(top - new_top)
            weights = jnp.exp2(scores - new_top)
            total = total * rescale + jnp.sum(weights, axis=1, keepdims=True)
            summed = summed * rescale + jnp.dot(
                weights.astype(jnp.bfloat16), far_values, preferred_element_type=jnp.float32
            )
            finished = summed / total
            result = finished if result is None else jnp.where(lane_head == head, finished, result)
        ready[index * block : (index + 1) * block, :] = result
        for peer in range(index * block // tokens, (index + 1) * block // tokens):

            @pl.when(me != peer)
            def _():
                backbound(peer, me).start()

            @pl.when(me == peer)
            def _():
                pltpu.make_async_copy(
                    ready.at[rows(peer), :], out_ref.at[:, columns(peer)], own_back
                ).start()

    for step in range(1, inner):
        backbound(me, lax.rem(me + step, inner)).wait_recv()
    pltpu.make_async_copy(ready.at[rows(me), :], out_ref.at[:, columns(me)], own_back).wait()
    for step in range(1, inner):
        peer = lax.rem(me + step, inner)
        for which in range(3):
            inbound(which, peer, me).wait_send()
        backbound(peer, me).wait_send()
    for other in range(1, outer):

        @pl.when(mine < other)
        def _():
            farbound(0, other, mine).wait_send()
            farbound(1, other, mine).wait_send()


def fused(queries, key_rows, value_rows, block):
    tokens, features = queries.shape
    inner = lax.axis_size("inner")
    outer = lax.axis_size("outer")
    slab = features // inner
    group = tokens * inner
    far_len = group // 4
    any_space = pl.BlockSpec(memory_space=pl.ANY)
    dims = (inner, outer, tokens, slab, features // HEADS, block)
    return pl.pallas_call(
        partial(fused_kernel, dims),
        out_shape=jax.ShapeDtypeStruct((tokens, features), jnp.float32),
        in_specs=[any_space] * 3,
        out_specs=any_space,
        scratch_shapes=[
            pltpu.VMEM((group, slab), jnp.bfloat16),
            pltpu.VMEM((group, slab), jnp.bfloat16),
            pltpu.VMEM((group, slab), jnp.bfloat16),
            pltpu.VMEM((outer - 1, far_len, slab), jnp.bfloat16),
            pltpu.VMEM((outer - 1, far_len, slab), jnp.bfloat16),
            pltpu.VMEM((far_len, slab), jnp.bfloat16),
            pltpu.VMEM((far_len, slab), jnp.bfloat16),
            pltpu.VMEM((group, slab), jnp.float32),
            pltpu.SemaphoreType.DMA((3, inner)),
            pltpu.SemaphoreType.DMA((3, inner)),
            pltpu.SemaphoreType.DMA((2, outer)),
            pltpu.SemaphoreType.DMA((2, outer)),
            pltpu.SemaphoreType.DMA((inner,)),
            pltpu.SemaphoreType.DMA((inner,)),
            pltpu.SemaphoreType.DMA((3,)),
            pltpu.SemaphoreType.DMA,
        ],
        compiler_params=pltpu.CompilerParams(collective_id=0, has_side_effects=True),
    )(queries, key_rows, value_rows)


def device_program(queries, key_rows, value_rows):
    tokens, features = queries.shape
    inner = lax.axis_size("inner")
    outer = lax.axis_size("outer")
    group = tokens * inner
    block = 2 * tokens
    slab = features // inner
    per_slab = HEADS // inner
    fits = (
        HEADS % inner == 0
        and outer > 1
        and inner > 1
        and per_slab > 0
        and 4 % max(per_slab, 1) == 0
        and slab % 128 == 0
        and tokens % 16 == 0
        and group % block == 0
        and group <= 1024
        and (outer - 1) * group // 4 <= 1024
    )
    if fits:
        return fused(queries, key_rows, value_rows, block)
    return on_device(queries, key_rows, value_rows)


def solution(mesh):
    placed = (P(("outer", "inner"), None), P(("outer", "inner"), None), P(("outer", "inner"), None))
    return jax.shard_map(
        device_program,
        mesh=mesh,
        in_specs=placed,
        out_specs=P(("outer", "inner"), None),
        check_vma=False,
    )
```

```python
import math
from functools import partial, reduce

import jax
import jax.numpy as jnp
import numpy as np
from jax import lax
from jax.experimental import pallas as pl
from jax.experimental.pallas import tpu as pltpu
from jax.sharding import PartitionSpec as P

HEADS = 16


FLOOR_SCORE = -1e30


def divisor_block(length, limit):
    extent = min(length, limit)
    while length % extent:
        extent -= 1
    return extent


def fresh_state(count, rows, width):
    return (
        jnp.full((count, rows), FLOOR_SCORE, jnp.float32),
        jnp.zeros((count, rows), jnp.float32),
        jnp.zeros((count, rows, width), jnp.float32),
    )


def finish_state(state):
    row_max, denominator, summed = state
    return (summed / denominator[..., None], row_max + jnp.log(denominator))


def online_step(state, query_rows, query_rank, key_rows, value_rows, key_rank):
    row_max, denominator, summed = state
    scale = query_rows.shape[-1] ** (-0.5)
    scores = (
        jnp.einsum("inh,ibh->inb", query_rows, key_rows, preferred_element_type=jnp.float32) * scale
    )
    scores = jnp.where(key_rank[None, None, :] <= query_rank[None, :, None], scores, FLOOR_SCORE)
    new_max = jnp.maximum(row_max, jnp.max(scores, axis=2))
    weights = jnp.exp(scores - new_max[..., None])
    rescale = jnp.exp(row_max - new_max)
    denominator = denominator * rescale + jnp.sum(weights, axis=2)
    summed = summed * rescale[..., None] + jnp.einsum(
        "inb,ibh->inh", weights.astype(jnp.bfloat16), value_rows, preferred_element_type=jnp.float32
    )
    return (new_max, denominator, summed)


def attend_keys(state, query_rows, query_rank, key_rows, value_rows, key_rank, stop=None):
    length = key_rows.shape[1]
    block = divisor_block(length, 512)

    def advance(index, carry):
        start = index * block
        piece_keys = lax.dynamic_slice_in_dim(key_rows, start, block, 1)
        piece_values = lax.dynamic_slice_in_dim(value_rows, start, block, 1)
        piece_rank = lax.dynamic_slice_in_dim(key_rank, start, block, 0)
        return online_step(carry, query_rows, query_rank, piece_keys, piece_values, piece_rank)

    upper = length // block if stop is None else stop
    return lax.fori_loop(0, upper, advance, state)


def attend(query_rows, query_rank, key_rows, value_rows, key_rank):
    count, length, width = query_rows.shape
    block = divisor_block(length, 512)
    steps = length // block
    query_split = query_rows.reshape(count, steps, block, width).swapaxes(0, 1)
    rank_split = query_rank.reshape(steps, block)

    def one_block(pieces):
        state = attend_keys(
            fresh_state(count, block, width),
            pieces[0],
            pieces[1],
            key_rows,
            value_rows,
            key_rank,
            pieces[2] + 1,
        )
        return finish_state(state)

    outputs, lses = lax.map(
        one_block, (query_split, rank_split, jnp.arange(steps, dtype=jnp.int32))
    )
    return (
        outputs.swapaxes(0, 1).reshape(count, length, width),
        lses.swapaxes(0, 1).reshape(count, length),
    )


def merge_levels(parts):
    row_max = reduce(jnp.maximum, [lse for _, lse in parts])
    weights = [jnp.exp(lse - row_max) for _, lse in parts]
    denominator = reduce(jnp.add, weights)
    summed = reduce(
        jnp.add, [weight[..., None] * output for weight, (output, _) in zip(weights, parts)]
    )
    return (summed / denominator[..., None], row_max + jnp.log(denominator))


def on_device(queries, key_rows, value_rows):
    tokens, features = queries.shape
    heads = HEADS
    width = features // heads
    outer_count = lax.axis_size("outer")
    inner_count = lax.axis_size("inner")
    outer_index = lax.axis_index("outer")
    inner_index = lax.axis_index("inner")
    per_device = 4 * heads // inner_count
    quarter = tokens // 4
    sixteenth = tokens // 16
    class_len = quarter * inner_count
    far_len = sixteenth * inner_count

    def to_items(array):
        return (
            array.reshape(quarter, 4, heads, width)
            .transpose(2, 1, 0, 3)
            .reshape(4 * heads, quarter, width)
        )

    local_ranks = jnp.arange(tokens, dtype=jnp.int32)
    head_major = [
        a.reshape(tokens, heads, width).transpose(1, 0, 2) for a in (queries, key_rows, value_rows)
    ]
    near_out, near_lse = attend(
        head_major[0], local_ranks, head_major[1], head_major[2], local_ranks
    )
    near_out = near_out.transpose(1, 0, 2)
    near_lse = near_lse.T
    item_index = inner_index * per_device + jnp.arange(per_device, dtype=jnp.int32)
    band = item_index // 16
    far_query_rank = outer_index * far_len + jnp.arange(far_len, dtype=jnp.int32)
    pick = np.array(
        [head * 16 + head // 4 * 4 + residue for head in range(heads) for residue in range(4)],
        np.int32,
    )

    def to_sixteen(array):
        spread = (
            array.reshape(sixteenth, 16, heads, width)
            .transpose(2, 1, 0, 3)
            .reshape(16 * heads, sixteenth, width)
        )
        return jnp.take(spread, pick, axis=0)

    gathered_k, gathered_v = (
        lax.all_gather(to_sixteen(key_rows), "outer", axis=1, tiled=True),
        lax.all_gather(to_sixteen(value_rows), "outer", axis=1, tiled=True),
    )
    mid_q, mid_k, mid_v, far_k, far_v = (
        lax.all_to_all(to_items(queries), "inner", split_axis=0, concat_axis=1, tiled=True),
        lax.all_to_all(to_items(key_rows), "inner", split_axis=0, concat_axis=1, tiled=True),
        lax.all_to_all(to_items(value_rows), "inner", split_axis=0, concat_axis=1, tiled=True),
        lax.all_to_all(gathered_k, "inner", split_axis=0, concat_axis=1, tiled=True),
        lax.all_to_all(gathered_v, "inner", split_axis=0, concat_axis=1, tiled=True),
    )
    split = mid_q.reshape(per_device, far_len, 4, width)
    picker = jnp.broadcast_to(band[:, None, None, None], (per_device, far_len, 1, width))
    far_q = jnp.take_along_axis(split, picker, axis=2)[:, :, 0, :]
    position = jnp.arange(far_k.shape[1], dtype=jnp.int32)
    far_key_rank = (
        position // sixteenth % outer_count * far_len
        + position // (outer_count * sixteenth) * sixteenth
        + position % sixteenth
    )
    far_state = attend_keys(
        fresh_state(per_device, far_len, width), far_q, far_query_rank, far_k, far_v, far_key_rank
    )
    far_out, far_lse = finish_state(far_state)
    class_ranks = jnp.arange(class_len, dtype=jnp.int32)
    mid_out, mid_lse = attend(mid_q, class_ranks, mid_k, mid_v, class_ranks)
    back_mid, back_mid_lse, back_far, back_far_lse = (
        lax.all_to_all(mid_out, "inner", split_axis=1, concat_axis=0, tiled=True),
        lax.all_to_all(mid_lse, "inner", split_axis=1, concat_axis=0, tiled=True),
        lax.all_to_all(far_out, "inner", split_axis=1, concat_axis=0, tiled=True),
        lax.all_to_all(far_lse, "inner", split_axis=1, concat_axis=0, tiled=True),
    )
    selector = np.array(
        [[band_index == head // 4 for band_index in range(4)] for head in range(heads)]
    )
    spread_out = jnp.where(
        selector[:, :, None, None, None], back_far.reshape(heads, 1, 4, sixteenth, width), 0.0
    )
    spread_lse = jnp.where(
        selector[:, :, None, None], back_far_lse.reshape(heads, 1, 4, sixteenth), FLOOR_SCORE
    )
    far_placed = (
        spread_out.reshape(heads, 16, sixteenth, width)
        .transpose(2, 1, 0, 3)
        .reshape(tokens, heads, width)
    )
    far_placed_lse = (
        spread_lse.reshape(heads, 16, sixteenth).transpose(2, 1, 0).reshape(tokens, heads)
    )
    placed = (
        back_mid.reshape(heads, 4, quarter, width)
        .transpose(2, 1, 0, 3)
        .reshape(tokens, heads, width)
    )
    placed_lse = back_mid_lse.reshape(heads, 4, quarter).transpose(2, 1, 0).reshape(tokens, heads)
    combined, _ = merge_levels(
        [(near_out, near_lse), (placed, placed_lse), (far_placed, far_placed_lse)]
    )
    return combined.reshape(tokens, features)


def fused_kernel(
    dims, q_ref, k_ref, v_ref, out_ref, q_held, k_held, v_held, q_buf, k_buf, v_buf, far_k, far_v, pick_k, pick_v, ready, ready_half, landed,
    in_send, in_recv, far_send, far_recv, back_send, back_recv, cross_send, cross_recv, own_sem, own_back, held_sem,
):
    inner, outer, tokens, slab, width, block = dims
    group = tokens * inner
    far_len = group // 4
    per_slab = slab // width
    me = lax.axis_index("inner")
    mine = lax.axis_index("outer")
    band = me * per_slab // 4
    sources = (k_ref, v_ref, q_ref)
    held = (k_held, v_held, q_held)
    half = inner // 2
    blocks = group // block
    order = [at for pair in zip(range(blocks // 2, blocks), range(blocks // 2)) for at in pair]
    buffers = (k_buf, v_buf, q_buf)

    def columns(index):
        return pl.ds(pl.multiple_of(index * slab, slab), slab)

    def rows(index):
        return pl.ds(pl.multiple_of(index * tokens, tokens), tokens)

    def inbound(which, peer, owner):
        return pltpu.make_async_remote_copy(
            src_ref=held[which].at[:, columns(peer)],
            dst_ref=buffers[which].at[rows(owner), :],
            send_sem=in_send.at[which, peer],
            recv_sem=in_recv.at[which, owner],
            device_id={"inner": peer},
            device_id_type=pl.DeviceIdType.MESH,
        )

    def farbound(which, peer, owner):
        return pltpu.make_async_remote_copy(
            src_ref=(pick_k, pick_v)[which],
            dst_ref=(far_k, far_v)[which].at[owner],
            send_sem=far_send.at[which, peer],
            recv_sem=far_recv.at[which, owner],
            device_id={"outer": peer},
            device_id_type=pl.DeviceIdType.MESH,
        )

    def backbound(peer, owner):
        return pltpu.make_async_remote_copy(
            src_ref=ready.at[rows(peer), :],
            dst_ref=out_ref.at[:, columns(owner)],
            send_sem=back_send.at[peer],
            recv_sem=back_recv.at[owner],
            device_id={"inner": peer},
            device_id_type=pl.DeviceIdType.MESH,
        )

    def crossbound(peer, owner):
        return pltpu.make_async_remote_copy(
            src_ref=ready_half.at[rows(peer), :],
            dst_ref=landed.at[:, columns(owner)],
            send_sem=cross_send.at[peer],
            recv_sem=cross_recv.at[owner],
            device_id={"inner": peer},
            device_id_type=pl.DeviceIdType.MESH,
        )

    def near(peer):
        return (me // half == peer // half) & (me != peer)

    own_in = [
        pltpu.make_async_copy(
            sources[which].at[:, columns(me)], buffers[which].at[rows(me), :], own_sem.at[which]
        )
        for which in range(3)
    ]
    own_held = [
        pltpu.make_async_copy(sources[which], held[which], held_sem.at[which]) for which in range(3)
    ]
    for copy in own_held + own_in:
        copy.start()
    barrier = pltpu.get_barrier_semaphore()
    for step in range(1, inner):
        pl.semaphore_signal(
            barrier, inc=1, device_id={"inner": lax.rem(me + step, inner)},
            device_id_type=pl.DeviceIdType.MESH,
        )
    for step in range(1, outer):
        pl.semaphore_signal(
            barrier, inc=1, device_id={"outer": lax.rem(mine + step, outer)},
            device_id_type=pl.DeviceIdType.MESH,
        )
    pl.semaphore_wait(barrier, inner + outer - 2)

    for which in range(3):
        own_held[which].wait()
        for step in range(1, inner):
            inbound(which, lax.rem(me + step, inner), me).start()

    for other in range(outer - 1):

        @pl.when(mine <= other)
        def _():
            far_k[other] = jnp.zeros((far_len, slab), jnp.bfloat16)
            far_v[other] = jnp.zeros((far_len, slab), jnp.bfloat16)

    query_at = lax.broadcasted_iota(jnp.int32, (block, block), 0)
    key_at = lax.broadcasted_iota(jnp.int32, (block, block), 1)
    levels = (query_at % 4 == key_at % 4).astype(jnp.int32) + (
        (query_at % 16 == key_at % 16) & (query_at % 16 // 4 == band)
    ).astype(jnp.int32)

    def log_count(count):
        return jnp.where(
            count == 0,
            FLOOR_SCORE,
            jnp.where(count == 1, 0.0, jnp.where(count == 2, 1.0, math.log2(3.0))),
        )

    below = log_count(levels)
    diagonal = log_count(
        jnp.where(
            key_at <= query_at, levels + (query_at // tokens == key_at // tokens).astype(jnp.int32), 0
        )
    )
    far_query = lax.broadcasted_iota(jnp.int32, (block, far_len), 0)
    far_key = lax.broadcasted_iota(jnp.int32, (block, far_len), 1)
    far_one = jnp.where(far_query % 16 == 4 * band + far_key % 4, 0.0, FLOOR_SCORE)
    far_table = jnp.concatenate(
        [jnp.where(other < mine, far_one, FLOOR_SCORE) for other in range(outer - 1)], axis=1
    )
    picked = lax.broadcasted_iota(jnp.int32, (far_len, group), 0)
    picker = jnp.where(
        lax.broadcasted_iota(jnp.int32, (far_len, group), 1)
        == picked // 4 * 16 + 4 * band + picked % 4,
        1.0,
        0.0,
    ).astype(jnp.bfloat16)

    def arrive(which):
        own_in[which].wait()
        for step in range(1, inner):
            inbound(which, me, lax.rem(me + step, inner)).wait_recv()

    for which in range(2):
        arrive(which)
        (pick_k, pick_v)[which][...] = jnp.dot(
            picker, buffers[which][...], preferred_element_type=jnp.float32
        ).astype(jnp.bfloat16)
        for other in range(1, outer):

            @pl.when(mine < other)
            def _():
                farbound(which, other, mine).start()

    factor = width ** (-0.5) * math.log2(math.e)
    lane_head = lax.broadcasted_iota(jnp.int32, (block, slab), 1) // width
    contract = (((1,), (1,)), ((), ()))

    def query_of(index, head):
        piece = q_buf[index * block : (index + 1) * block, :]
        return jnp.where(lane_head == head, piece, jnp.zeros_like(piece))

    own_in[2].wait()
    states = {}
    for index in order:
        for peer in range(index * block // tokens, (index + 1) * block // tokens):

            @pl.when(me != peer)
            def _():
                inbound(2, me, peer).wait_recv()

        reach = (index + 1) * block
        table = jnp.concatenate([below] * index + [diagonal], axis=1)
        for head in range(per_slab):
            scores = lax.dot_general(
                query_of(index, head), k_buf[:reach, :], contract,
                preferred_element_type=jnp.float32,
            )
            scores = scores * factor + table
            top = jnp.max(scores, axis=1, keepdims=True)
            weights = jnp.exp2(scores - top)
            total = jnp.sum(weights, axis=1, keepdims=True)
            summed = jnp.dot(
                weights.astype(jnp.bfloat16), v_buf[:reach, :], preferred_element_type=jnp.float32
            )
            states[index, head] = (top, total, summed)

    for other in range(outer - 1):

        @pl.when(mine > other)
        def _():
            farbound(0, mine, other).wait_recv()
            farbound(1, mine, other).wait_recv()

    far_keys = far_k[...].reshape((outer - 1) * far_len, slab)
    far_values = far_v[...].reshape((outer - 1) * far_len, slab)
    for index in order:
        result = None
        for head in range(per_slab):
            top, total, summed = states[index, head]
            scores = lax.dot_general(
                query_of(index, head), far_keys, contract, preferred_element_type=jnp.float32
            )
            scores = scores * factor + far_table
            new_top = jnp.maximum(top, jnp.max(scores, axis=1, keepdims=True))
            rescale = jnp.exp2(top - new_top)
            weights = jnp.exp2(scores - new_top)
            total = total * rescale + jnp.sum(weights, axis=1, keepdims=True)
            summed = summed * rescale + jnp.dot(
                weights.astype(jnp.bfloat16), far_values, preferred_element_type=jnp.float32
            )
            finished = summed / total
            result = finished if result is None else jnp.where(lane_head == head, finished, result)
        ready[index * block : (index + 1) * block, :] = result
        ready_half[index * block : (index + 1) * block, :] = result.astype(jnp.bfloat16)
        for peer in range(index * block // tokens, (index + 1) * block // tokens):

            @pl.when(me // half != peer // half)
            def _():
                crossbound(peer, me).start()

            @pl.when(near(peer))
            def _():
                backbound(peer, me).start()

            @pl.when(me == peer)
            def _():
                pltpu.make_async_copy(
                    ready.at[rows(peer), :], out_ref.at[:, columns(peer)], own_back
                ).start()

    for owner in range(inner):

        @pl.when(me // half != owner // half)
        def _():
            crossbound(me, owner).wait_recv()
            place = slice(owner * slab, (owner + 1) * slab)
            out_ref[:, place] = landed[:, place].astype(jnp.float32)

    for owner in range(inner):

        @pl.when(near(owner))
        def _():
            backbound(me, owner).wait_recv()

    pltpu.make_async_copy(ready.at[rows(me), :], out_ref.at[:, columns(me)], own_back).wait()
    for step in range(1, inner):
        peer = lax.rem(me + step, inner)
        for which in range(3):
            inbound(which, peer, me).wait_send()

        @pl.when(me // half != peer // half)
        def _():
            crossbound(peer, me).wait_send()

        @pl.when(near(peer))
        def _():
            backbound(peer, me).wait_send()

    for other in range(1, outer):

        @pl.when(mine < other)
        def _():
            farbound(0, other, mine).wait_send()
            farbound(1, other, mine).wait_send()


def fused(queries, key_rows, value_rows, block):
    tokens, features = queries.shape
    inner = lax.axis_size("inner")
    outer = lax.axis_size("outer")
    slab = features // inner
    group = tokens * inner
    far_len = group // 4
    any_space = pl.BlockSpec(memory_space=pl.ANY)
    dims = (inner, outer, tokens, slab, features // HEADS, block)
    return pl.pallas_call(
        partial(fused_kernel, dims),
        out_shape=pltpu.VMEM((tokens, features), jnp.float32),
        in_specs=[any_space] * 3,
        out_specs=pl.BlockSpec(memory_space=pltpu.VMEM),
        scratch_shapes=[
            pltpu.VMEM((tokens, features), jnp.bfloat16),
            pltpu.VMEM((tokens, features), jnp.bfloat16),
            pltpu.VMEM((tokens, features), jnp.bfloat16),
            pltpu.VMEM((group, slab), jnp.bfloat16),
            pltpu.VMEM((group, slab), jnp.bfloat16),
            pltpu.VMEM((group, slab), jnp.bfloat16),
            pltpu.VMEM((outer - 1, far_len, slab), jnp.bfloat16),
            pltpu.VMEM((outer - 1, far_len, slab), jnp.bfloat16),
            pltpu.VMEM((far_len, slab), jnp.bfloat16),
            pltpu.VMEM((far_len, slab), jnp.bfloat16),
            pltpu.VMEM((group, slab), jnp.float32),
            pltpu.VMEM((group, slab), jnp.bfloat16),
            pltpu.VMEM((tokens, features), jnp.bfloat16),
            pltpu.SemaphoreType.DMA((3, inner)),
            pltpu.SemaphoreType.DMA((3, inner)),
            pltpu.SemaphoreType.DMA((2, outer)),
            pltpu.SemaphoreType.DMA((2, outer)),
            pltpu.SemaphoreType.DMA((inner,)),
            pltpu.SemaphoreType.DMA((inner,)),
            pltpu.SemaphoreType.DMA((inner,)),
            pltpu.SemaphoreType.DMA((inner,)),
            pltpu.SemaphoreType.DMA((3,)),
            pltpu.SemaphoreType.DMA,
            pltpu.SemaphoreType.DMA((3,)),
        ],
        compiler_params=pltpu.CompilerParams(collective_id=0, has_side_effects=True),
    )(queries, key_rows, value_rows)


def device_program(queries, key_rows, value_rows):
    tokens, features = queries.shape
    inner = lax.axis_size("inner")
    outer = lax.axis_size("outer")
    group = tokens * inner
    block = 2 * tokens
    slab = features // inner
    per_slab = HEADS // inner
    fits = (
        HEADS % inner == 0
        and outer > 1
        and inner % 2 == 0
        and per_slab > 0
        and 4 % max(per_slab, 1) == 0
        and slab % 128 == 0
        and tokens % 16 == 0
        and group % (2 * block) == 0
        and group <= 1024
        and (outer - 1) * group // 4 <= 1024
    )
    if fits:
        return fused(queries, key_rows, value_rows, block)
    return on_device(queries, key_rows, value_rows)


def solution(mesh):
    placed = (P(("outer", "inner"), None), P(("outer", "inner"), None), P(("outer", "inner"), None))
    return jax.shard_map(
        device_program,
        mesh=mesh,
        in_specs=placed,
        out_specs=P(("outer", "inner"), None),
        check_vma=False,
    )
```

```python
import math
from functools import partial, reduce

import jax
import jax.numpy as jnp
import numpy as np
from jax import lax
from jax.experimental import pallas as pl
from jax.experimental.pallas import tpu as pltpu
from jax.sharding import PartitionSpec as P

HEADS = 16


FLOOR_SCORE = -1e30


def divisor_block(length, limit):
    extent = min(length, limit)
    while length % extent:
        extent -= 1
    return extent


def fresh_state(count, rows, width):
    return (
        jnp.full((count, rows), FLOOR_SCORE, jnp.float32),
        jnp.zeros((count, rows), jnp.float32),
        jnp.zeros((count, rows, width), jnp.float32),
    )


def finish_state(state):
    row_max, denominator, summed = state
    return (summed / denominator[..., None], row_max + jnp.log(denominator))


def online_step(state, query_rows, query_rank, key_rows, value_rows, key_rank):
    row_max, denominator, summed = state
    scale = query_rows.shape[-1] ** (-0.5)
    scores = (
        jnp.einsum("inh,ibh->inb", query_rows, key_rows, preferred_element_type=jnp.float32) * scale
    )
    scores = jnp.where(key_rank[None, None, :] <= query_rank[None, :, None], scores, FLOOR_SCORE)
    new_max = jnp.maximum(row_max, jnp.max(scores, axis=2))
    weights = jnp.exp(scores - new_max[..., None])
    rescale = jnp.exp(row_max - new_max)
    denominator = denominator * rescale + jnp.sum(weights, axis=2)
    summed = summed * rescale[..., None] + jnp.einsum(
        "inb,ibh->inh", weights.astype(jnp.bfloat16), value_rows, preferred_element_type=jnp.float32
    )
    return (new_max, denominator, summed)


def attend_keys(state, query_rows, query_rank, key_rows, value_rows, key_rank, stop=None):
    length = key_rows.shape[1]
    block = divisor_block(length, 512)

    def advance(index, carry):
        start = index * block
        piece_keys = lax.dynamic_slice_in_dim(key_rows, start, block, 1)
        piece_values = lax.dynamic_slice_in_dim(value_rows, start, block, 1)
        piece_rank = lax.dynamic_slice_in_dim(key_rank, start, block, 0)
        return online_step(carry, query_rows, query_rank, piece_keys, piece_values, piece_rank)

    upper = length // block if stop is None else stop
    return lax.fori_loop(0, upper, advance, state)


def attend(query_rows, query_rank, key_rows, value_rows, key_rank):
    count, length, width = query_rows.shape
    block = divisor_block(length, 512)
    steps = length // block
    query_split = query_rows.reshape(count, steps, block, width).swapaxes(0, 1)
    rank_split = query_rank.reshape(steps, block)

    def one_block(pieces):
        state = attend_keys(
            fresh_state(count, block, width),
            pieces[0],
            pieces[1],
            key_rows,
            value_rows,
            key_rank,
            pieces[2] + 1,
        )
        return finish_state(state)

    outputs, lses = lax.map(
        one_block, (query_split, rank_split, jnp.arange(steps, dtype=jnp.int32))
    )
    return (
        outputs.swapaxes(0, 1).reshape(count, length, width),
        lses.swapaxes(0, 1).reshape(count, length),
    )


def merge_levels(parts):
    row_max = reduce(jnp.maximum, [lse for _, lse in parts])
    weights = [jnp.exp(lse - row_max) for _, lse in parts]
    denominator = reduce(jnp.add, weights)
    summed = reduce(
        jnp.add, [weight[..., None] * output for weight, (output, _) in zip(weights, parts)]
    )
    return (summed / denominator[..., None], row_max + jnp.log(denominator))


def on_device(queries, key_rows, value_rows):
    tokens, features = queries.shape
    heads = HEADS
    width = features // heads
    outer_count = lax.axis_size("outer")
    inner_count = lax.axis_size("inner")
    outer_index = lax.axis_index("outer")
    inner_index = lax.axis_index("inner")
    per_device = 4 * heads // inner_count
    quarter = tokens // 4
    sixteenth = tokens // 16
    class_len = quarter * inner_count
    far_len = sixteenth * inner_count

    def to_items(array):
        return (
            array.reshape(quarter, 4, heads, width)
            .transpose(2, 1, 0, 3)
            .reshape(4 * heads, quarter, width)
        )

    local_ranks = jnp.arange(tokens, dtype=jnp.int32)
    head_major = [
        a.reshape(tokens, heads, width).transpose(1, 0, 2) for a in (queries, key_rows, value_rows)
    ]
    near_out, near_lse = attend(
        head_major[0], local_ranks, head_major[1], head_major[2], local_ranks
    )
    near_out = near_out.transpose(1, 0, 2)
    near_lse = near_lse.T
    item_index = inner_index * per_device + jnp.arange(per_device, dtype=jnp.int32)
    band = item_index // 16
    far_query_rank = outer_index * far_len + jnp.arange(far_len, dtype=jnp.int32)
    pick = np.array(
        [head * 16 + head // 4 * 4 + residue for head in range(heads) for residue in range(4)],
        np.int32,
    )

    def to_sixteen(array):
        spread = (
            array.reshape(sixteenth, 16, heads, width)
            .transpose(2, 1, 0, 3)
            .reshape(16 * heads, sixteenth, width)
        )
        return jnp.take(spread, pick, axis=0)

    gathered_k, gathered_v = (
        lax.all_gather(to_sixteen(key_rows), "outer", axis=1, tiled=True),
        lax.all_gather(to_sixteen(value_rows), "outer", axis=1, tiled=True),
    )
    mid_q, mid_k, mid_v, far_k, far_v = (
        lax.all_to_all(to_items(queries), "inner", split_axis=0, concat_axis=1, tiled=True),
        lax.all_to_all(to_items(key_rows), "inner", split_axis=0, concat_axis=1, tiled=True),
        lax.all_to_all(to_items(value_rows), "inner", split_axis=0, concat_axis=1, tiled=True),
        lax.all_to_all(gathered_k, "inner", split_axis=0, concat_axis=1, tiled=True),
        lax.all_to_all(gathered_v, "inner", split_axis=0, concat_axis=1, tiled=True),
    )
    split = mid_q.reshape(per_device, far_len, 4, width)
    picker = jnp.broadcast_to(band[:, None, None, None], (per_device, far_len, 1, width))
    far_q = jnp.take_along_axis(split, picker, axis=2)[:, :, 0, :]
    position = jnp.arange(far_k.shape[1], dtype=jnp.int32)
    far_key_rank = (
        position // sixteenth % outer_count * far_len
        + position // (outer_count * sixteenth) * sixteenth
        + position % sixteenth
    )
    far_state = attend_keys(
        fresh_state(per_device, far_len, width), far_q, far_query_rank, far_k, far_v, far_key_rank
    )
    far_out, far_lse = finish_state(far_state)
    class_ranks = jnp.arange(class_len, dtype=jnp.int32)
    mid_out, mid_lse = attend(mid_q, class_ranks, mid_k, mid_v, class_ranks)
    back_mid, back_mid_lse, back_far, back_far_lse = (
        lax.all_to_all(mid_out, "inner", split_axis=1, concat_axis=0, tiled=True),
        lax.all_to_all(mid_lse, "inner", split_axis=1, concat_axis=0, tiled=True),
        lax.all_to_all(far_out, "inner", split_axis=1, concat_axis=0, tiled=True),
        lax.all_to_all(far_lse, "inner", split_axis=1, concat_axis=0, tiled=True),
    )
    selector = np.array(
        [[band_index == head // 4 for band_index in range(4)] for head in range(heads)]
    )
    spread_out = jnp.where(
        selector[:, :, None, None, None], back_far.reshape(heads, 1, 4, sixteenth, width), 0.0
    )
    spread_lse = jnp.where(
        selector[:, :, None, None], back_far_lse.reshape(heads, 1, 4, sixteenth), FLOOR_SCORE
    )
    far_placed = (
        spread_out.reshape(heads, 16, sixteenth, width)
        .transpose(2, 1, 0, 3)
        .reshape(tokens, heads, width)
    )
    far_placed_lse = (
        spread_lse.reshape(heads, 16, sixteenth).transpose(2, 1, 0).reshape(tokens, heads)
    )
    placed = (
        back_mid.reshape(heads, 4, quarter, width)
        .transpose(2, 1, 0, 3)
        .reshape(tokens, heads, width)
    )
    placed_lse = back_mid_lse.reshape(heads, 4, quarter).transpose(2, 1, 0).reshape(tokens, heads)
    combined, _ = merge_levels(
        [(near_out, near_lse), (placed, placed_lse), (far_placed, far_placed_lse)]
    )
    return combined.reshape(tokens, features)


def fused_kernel(
    dims, q_ref, k_ref, v_ref, out_ref, q_held, k_held, v_held, q_buf, k_buf, v_buf, far_k, far_v, pick_k, pick_v, ready, ready_half, landed,
    in_send, in_recv, far_send, far_recv, back_send, back_recv, cross_send, cross_recv, own_sem, own_back, held_sem,
):
    inner, outer, tokens, slab, width, block = dims
    group = tokens * inner
    far_len = group // 4
    per_slab = slab // width
    me = lax.axis_index("inner")
    mine = lax.axis_index("outer")
    band = me * per_slab // 4
    sources = (k_ref, v_ref, q_ref)
    held = (k_held, v_held, q_held)
    half = inner // 2
    order = range(group // block)
    buffers = (k_buf, v_buf, q_buf)

    def columns(index):
        return pl.ds(pl.multiple_of(index * slab, slab), slab)

    def rows(index):
        return pl.ds(pl.multiple_of(index * tokens, tokens), tokens)

    def inbound(which, peer, owner):
        return pltpu.make_async_remote_copy(
            src_ref=held[which].at[:, columns(peer)],
            dst_ref=buffers[which].at[rows(owner), :],
            send_sem=in_send.at[which, peer],
            recv_sem=in_recv.at[which, owner],
            device_id={"inner": peer},
            device_id_type=pl.DeviceIdType.MESH,
        )

    def farbound(which, peer, owner):
        return pltpu.make_async_remote_copy(
            src_ref=(pick_k, pick_v)[which],
            dst_ref=(far_k, far_v)[which].at[owner],
            send_sem=far_send.at[which, peer],
            recv_sem=far_recv.at[which, owner],
            device_id={"outer": peer},
            device_id_type=pl.DeviceIdType.MESH,
        )

    def backbound(peer, owner):
        return pltpu.make_async_remote_copy(
            src_ref=ready.at[rows(peer), :],
            dst_ref=out_ref.at[:, columns(owner)],
            send_sem=back_send.at[peer],
            recv_sem=back_recv.at[owner],
            device_id={"inner": peer},
            device_id_type=pl.DeviceIdType.MESH,
        )

    def crossbound(peer, owner):
        return pltpu.make_async_remote_copy(
            src_ref=ready_half.at[rows(peer), :],
            dst_ref=landed.at[:, columns(owner)],
            send_sem=cross_send.at[peer],
            recv_sem=cross_recv.at[owner],
            device_id={"inner": peer},
            device_id_type=pl.DeviceIdType.MESH,
        )

    def near(peer):
        return (me // half == peer // half) & (me != peer)

    own_in = [
        pltpu.make_async_copy(
            sources[which].at[:, columns(me)], buffers[which].at[rows(me), :], own_sem.at[which]
        )
        for which in range(3)
    ]
    own_held = [
        pltpu.make_async_copy(sources[which], held[which], held_sem.at[which]) for which in range(3)
    ]
    for copy in own_held + own_in:
        copy.start()
    barrier = pltpu.get_barrier_semaphore()
    for step in range(1, inner):
        pl.semaphore_signal(
            barrier, inc=1, device_id={"inner": lax.rem(me + step, inner)},
            device_id_type=pl.DeviceIdType.MESH,
        )
    for step in range(1, outer):
        pl.semaphore_signal(
            barrier, inc=1, device_id={"outer": lax.rem(mine + step, outer)},
            device_id_type=pl.DeviceIdType.MESH,
        )
    pl.semaphore_wait(barrier, inner + outer - 2)

    for which in range(3):
        own_held[which].wait()
        for step in range(1, inner):
            inbound(which, lax.rem(me + step, inner), me).start()

    for other in range(outer - 1):

        @pl.when(mine <= other)
        def _():
            far_k[other] = jnp.zeros((far_len, slab), jnp.bfloat16)
            far_v[other] = jnp.zeros((far_len, slab), jnp.bfloat16)

    query_at = lax.broadcasted_iota(jnp.int32, (block, block), 0)
    key_at = lax.broadcasted_iota(jnp.int32, (block, block), 1)
    levels = (query_at % 4 == key_at % 4).astype(jnp.int32) + (
        (query_at % 16 == key_at % 16) & (query_at % 16 // 4 == band)
    ).astype(jnp.int32)

    def log_count(count):
        return jnp.where(
            count == 0,
            FLOOR_SCORE,
            jnp.where(count == 1, 0.0, jnp.where(count == 2, 1.0, math.log2(3.0))),
        )

    below = log_count(levels)
    diagonal = log_count(
        jnp.where(
            key_at <= query_at, levels + (query_at // tokens == key_at // tokens).astype(jnp.int32), 0
        )
    )
    far_query = lax.broadcasted_iota(jnp.int32, (block, far_len), 0)
    far_key = lax.broadcasted_iota(jnp.int32, (block, far_len), 1)
    far_one = jnp.where(far_query % 16 == 4 * band + far_key % 4, 0.0, FLOOR_SCORE)
    far_table = jnp.concatenate(
        [jnp.where(other < mine, far_one, FLOOR_SCORE) for other in range(outer - 1)], axis=1
    )
    picked = lax.broadcasted_iota(jnp.int32, (far_len, group), 0)
    picker = jnp.where(
        lax.broadcasted_iota(jnp.int32, (far_len, group), 1)
        == picked // 4 * 16 + 4 * band + picked % 4,
        1.0,
        0.0,
    ).astype(jnp.bfloat16)

    def arrive(which):
        own_in[which].wait()
        for step in range(1, inner):
            inbound(which, me, lax.rem(me + step, inner)).wait_recv()

    for which in range(2):
        arrive(which)
        (pick_k, pick_v)[which][...] = jnp.dot(
            picker, buffers[which][...], preferred_element_type=jnp.float32
        ).astype(jnp.bfloat16)
        for other in range(1, outer):

            @pl.when(mine < other)
            def _():
                farbound(which, other, mine).start()

    factor = width ** (-0.5) * math.log2(math.e)
    lane_head = lax.broadcasted_iota(jnp.int32, (block, slab), 1) // width
    contract = (((1,), (1,)), ((), ()))

    def query_of(index, head):
        piece = q_buf[index * block : (index + 1) * block, :]
        return jnp.where(lane_head == head, piece, jnp.zeros_like(piece))

    own_in[2].wait()
    states = {}
    for index in order:
        for peer in range(index * block // tokens, (index + 1) * block // tokens):

            @pl.when(me != peer)
            def _():
                inbound(2, me, peer).wait_recv()

        reach = (index + 1) * block
        table = jnp.concatenate([below] * index + [diagonal], axis=1)
        for head in range(per_slab):
            scores = lax.dot_general(
                query_of(index, head), k_buf[:reach, :], contract,
                preferred_element_type=jnp.float32,
            )
            scores = scores * factor + table
            top = jnp.max(scores, axis=1, keepdims=True)
            weights = jnp.exp2(scores - top)
            total = jnp.sum(weights, axis=1, keepdims=True)
            summed = jnp.dot(
                weights.astype(jnp.bfloat16), v_buf[:reach, :], preferred_element_type=jnp.float32
            )
            states[index, head] = (top, total, summed)

    for other in range(outer - 1):

        @pl.when(mine > other)
        def _():
            farbound(0, mine, other).wait_recv()
            farbound(1, mine, other).wait_recv()

    far_keys = far_k[...].reshape((outer - 1) * far_len, slab)
    far_values = far_v[...].reshape((outer - 1) * far_len, slab)
    for index in order:
        result = None
        for head in range(per_slab):
            top, total, summed = states[index, head]
            scores = lax.dot_general(
                query_of(index, head), far_keys, contract, preferred_element_type=jnp.float32
            )
            scores = scores * factor + far_table
            new_top = jnp.maximum(top, jnp.max(scores, axis=1, keepdims=True))
            rescale = jnp.exp2(top - new_top)
            weights = jnp.exp2(scores - new_top)
            total = total * rescale + jnp.sum(weights, axis=1, keepdims=True)
            summed = summed * rescale + jnp.dot(
                weights.astype(jnp.bfloat16), far_values, preferred_element_type=jnp.float32
            )
            finished = summed / total
            result = finished if result is None else jnp.where(lane_head == head, finished, result)
        ready[index * block : (index + 1) * block, :] = result
        ready_half[index * block : (index + 1) * block, :] = result.astype(jnp.bfloat16)
        for peer in range(index * block // tokens, (index + 1) * block // tokens):

            @pl.when(me // half != peer // half)
            def _():
                crossbound(peer, me).start()

            @pl.when(near(peer))
            def _():
                backbound(peer, me).start()

            @pl.when(me == peer)
            def _():
                pltpu.make_async_copy(
                    ready.at[rows(peer), :], out_ref.at[:, columns(peer)], own_back
                ).start()

    for owner in range(inner):

        @pl.when(me // half != owner // half)
        def _():
            crossbound(me, owner).wait_recv()
            place = slice(owner * slab, (owner + 1) * slab)
            out_ref[:, place] = landed[:, place].astype(jnp.float32)

    for owner in range(inner):

        @pl.when(near(owner))
        def _():
            backbound(me, owner).wait_recv()

    pltpu.make_async_copy(ready.at[rows(me), :], out_ref.at[:, columns(me)], own_back).wait()
    for step in range(1, inner):
        peer = lax.rem(me + step, inner)
        for which in range(3):
            inbound(which, peer, me).wait_send()

        @pl.when(me // half != peer // half)
        def _():
            crossbound(peer, me).wait_send()

        @pl.when(near(peer))
        def _():
            backbound(peer, me).wait_send()

    for other in range(1, outer):

        @pl.when(mine < other)
        def _():
            farbound(0, other, mine).wait_send()
            farbound(1, other, mine).wait_send()


def fused(queries, key_rows, value_rows, block):
    tokens, features = queries.shape
    inner = lax.axis_size("inner")
    outer = lax.axis_size("outer")
    slab = features // inner
    group = tokens * inner
    far_len = group // 4
    any_space = pl.BlockSpec(memory_space=pl.ANY)
    dims = (inner, outer, tokens, slab, features // HEADS, block)
    return pl.pallas_call(
        partial(fused_kernel, dims),
        out_shape=pltpu.VMEM((tokens, features), jnp.float32),
        in_specs=[any_space] * 3,
        out_specs=pl.BlockSpec(memory_space=pltpu.VMEM),
        scratch_shapes=[
            pltpu.VMEM((tokens, features), jnp.bfloat16),
            pltpu.VMEM((tokens, features), jnp.bfloat16),
            pltpu.VMEM((tokens, features), jnp.bfloat16),
            pltpu.VMEM((group, slab), jnp.bfloat16),
            pltpu.VMEM((group, slab), jnp.bfloat16),
            pltpu.VMEM((group, slab), jnp.bfloat16),
            pltpu.VMEM((outer - 1, far_len, slab), jnp.bfloat16),
            pltpu.VMEM((outer - 1, far_len, slab), jnp.bfloat16),
            pltpu.VMEM((far_len, slab), jnp.bfloat16),
            pltpu.VMEM((far_len, slab), jnp.bfloat16),
            pltpu.VMEM((group, slab), jnp.float32),
            pltpu.VMEM((group, slab), jnp.bfloat16),
            pltpu.VMEM((tokens, features), jnp.bfloat16),
            pltpu.SemaphoreType.DMA((3, inner)),
            pltpu.SemaphoreType.DMA((3, inner)),
            pltpu.SemaphoreType.DMA((2, outer)),
            pltpu.SemaphoreType.DMA((2, outer)),
            pltpu.SemaphoreType.DMA((inner,)),
            pltpu.SemaphoreType.DMA((inner,)),
            pltpu.SemaphoreType.DMA((inner,)),
            pltpu.SemaphoreType.DMA((inner,)),
            pltpu.SemaphoreType.DMA((3,)),
            pltpu.SemaphoreType.DMA,
            pltpu.SemaphoreType.DMA((3,)),
        ],
        compiler_params=pltpu.CompilerParams(collective_id=0, has_side_effects=True),
    )(queries, key_rows, value_rows)


def device_program(queries, key_rows, value_rows):
    tokens, features = queries.shape
    inner = lax.axis_size("inner")
    outer = lax.axis_size("outer")
    group = tokens * inner
    block = 2 * tokens
    slab = features // inner
    per_slab = HEADS // inner
    fits = (
        HEADS % inner == 0
        and outer > 1
        and inner % 2 == 0
        and per_slab > 0
        and 4 % max(per_slab, 1) == 0
        and slab % 128 == 0
        and tokens % 16 == 0
        and group % block == 0
        and group <= 1024
        and (outer - 1) * group // 4 <= 1024
    )
    if fits:
        return fused(queries, key_rows, value_rows, block)
    return on_device(queries, key_rows, value_rows)


def solution(mesh):
    placed = (P(("outer", "inner"), None), P(("outer", "inner"), None), P(("outer", "inner"), None))
    return jax.shard_map(
        device_program,
        mesh=mesh,
        in_specs=placed,
        out_specs=P(("outer", "inner"), None),
        check_vma=False,
    )
```
